256 devices in a mesh: head: 8 (over x, core), seq: 32 (over y, z).
Axes of the slice: x: 4, y: 4, z: 8, core: 2. Of those that a mesh axis runs over, the one named last changes fastest.
Arguments:
- queries: bfloat16 [49152, 4096], P('seq', 'head'), may hold values from -32 to 32
- key_rows: bfloat16 [49152, 4096], P('seq', 'head'), may hold values from -32 to 32
- value_rows: bfloat16 [49152, 4096], P('seq', 'head'), may hold values from -6 to 6
- learn_rates: bfloat16 [49152, 8], P('seq', 'head'), may hold values from 0.00012683868 to 0.0012741089
- gate_fast: float32 [8, 512, 512], P('head'), may hold values from -0.25 to 0.25
- down_fast: float32 [8, 512, 512], P('head'), may hold values from -0.25 to 0.25
- up_fast: float32 [8, 512, 512], P('head'), may hold values from -0.25 to 0.25
Outputs:
- mixed: bfloat16 [49152, 4096], P('seq', 'head')
The draws below stay inside these ranges and needn't reach their ends.
All inputs are finite; a program needn't handle non-finite values.
Results may differ from the reference program's by a relative error of at most 0.024.
Values may be sent and summed in bfloat16 or wider, within the bound.
A program may use at most 128 MiB of HBM per device.

```python
import math
import jax
import jax.numpy as jnp
from jax import lax

H = 8
DH = 512
AH = 128
WINDOW = 512
D = 4096
TOKENS = 49152
GROUP = 24576


def paired_rows(key):
    base_key = jax.random.fold_in(key, 4242)
    first_key, second_key = jax.random.split(base_key, 2)
    query_all = jax.random.truncated_normal(first_key, -4.0, 4.0, (TOKENS, D), jnp.float32)
    key_all = jax.random.truncated_normal(second_key, -4.0, 4.0, (TOKENS, D), jnp.float32)
    return (query_all, key_all)


def draw_queries(key, part):
    return paired_rows(key)[0].astype(jnp.bfloat16)


def draw_key_rows(key, part):
    return paired_rows(key)[1].astype(jnp.bfloat16)


def level_of(stream_key, dims, cuts, least, top_value):
    def one(axis_at, parts):
        steps = jax.random.uniform(jax.random.fold_in(jax.random.fold_in(stream_key, 6), axis_at), (parts,), jnp.float32, least / len(cuts), top_value / len(cuts))
        return jnp.repeat(jnp.exp(steps), dims[axis_at] // parts).reshape((-1,) + (1,) * (len(dims) - axis_at - 1))

    factor_of = one(*cuts[0])
    for cut in cuts[1:]:
        factor_of = factor_of * one(*cut)
    return factor_of


def normal_values(stream_key, dims, spread, most, cuts=(), kind=jnp.bfloat16):
    values = spread * jax.random.normal(stream_key, dims, jnp.float32)
    if cuts:
        values = values * level_of(stream_key, dims, cuts, -0.22, 0.18)
    return jnp.clip(values, -most, most).astype(kind)


def setup_inputs(seed: int = 0) -> dict:
    seeds = jax.random.split(jax.random.key(seed), 8)
    queries = draw_queries(jax.random.fold_in(seeds[7], 71), 0)
    key_rows = draw_key_rows(jax.random.fold_in(seeds[7], 71), 0)
    value_rows = normal_values(seeds[2], (TOKENS, D), 1.0, 6.0, ((0, 32), (1, 8)))
    learn_rates = jnp.clip(jnp.exp(math.log(0.0012741089) - 2.3070862 * jax.random.uniform(seeds[3], (TOKENS, H), jnp.float32) ** level_of(seeds[3], (TOKENS, H), ((0, 32), (1, 8)), -0.2, 0.2)), 0.00012683868, 0.0012741089).astype(jnp.bfloat16)
    gate_fast = normal_values(seeds[4], (H, DH, DH), DH ** -0.5, 0.25, ((0, 8),), jnp.float32)
    down_fast = normal_values(seeds[5], (H, DH, DH), DH ** -0.5, 0.25, ((0, 8),), jnp.float32)
    up_fast = normal_values(seeds[6], (H, DH, DH), DH ** -0.5, 0.25, ((0, 8),), jnp.float32)
    return dict(queries=queries, key_rows=key_rows, value_rows=value_rows, learn_rates=learn_rates, gate_fast=gate_fast, down_fast=down_fast, up_fast=up_fast)


EPSILON = 1e-06

def norm_rows(values_in):
    as_float = values_in.astype(jnp.float32)
    return (as_float / jnp.sqrt(lax.optimization_barrier(jnp.mean(as_float * as_float, axis=-1, keepdims=True)) + EPSILON)).astype(jnp.bfloat16)

def fast_terms(fast_bf, key_norm, value_slice, rate_slice):
    gate_w, down_w, up_w = fast_bf
    gate_pre = jnp.dot(key_norm, gate_w, preferred_element_type=jnp.float32)
    up_pre = jnp.dot(key_norm, up_w, preferred_element_type=jnp.float32)
    sigmoid_gate = jax.nn.sigmoid(gate_pre)
    gate_act = gate_pre * sigmoid_gate
    hidden = (gate_act * up_pre).astype(jnp.bfloat16)
    scaled_val = (rate_slice.astype(jnp.float32)[:, None] * value_slice.astype(jnp.float32)).astype(jnp.bfloat16)
    hidden_grad = -jnp.dot(scaled_val, down_w.T, preferred_element_type=jnp.float32)
    gate_grad = (hidden_grad * up_pre * sigmoid_gate * (1.0 + gate_pre * (1.0 - sigmoid_gate))).astype(jnp.bfloat16)
    up_grad = (hidden_grad * gate_act).astype(jnp.bfloat16)
    gate_term = jnp.dot(key_norm.T, gate_grad, preferred_element_type=jnp.float32)
    down_term = -jnp.dot(hidden.T, scaled_val, preferred_element_type=jnp.float32)
    up_term = jnp.dot(key_norm.T, up_grad, preferred_element_type=jnp.float32)
    return (gate_term, down_term, up_term)

def rescale(weight, moved):
    target_norm = jnp.sqrt(lax.optimization_barrier(jnp.sum(weight * weight, axis=-2, keepdims=True)))
    return moved * target_norm / jnp.sqrt(lax.optimization_barrier(jnp.sum(moved * moved, axis=-2, keepdims=True)) + EPSILON)

def apply_fast(fast_bf, query_norm):
    gate_w, down_w, up_w = fast_bf
    gate_pre = jnp.dot(query_norm, gate_w, preferred_element_type=jnp.float32)
    up_pre = jnp.dot(query_norm, up_w, preferred_element_type=jnp.float32)
    hidden = (gate_pre * jax.nn.sigmoid(gate_pre) * up_pre).astype(jnp.bfloat16)
    return jnp.dot(hidden, down_w, preferred_element_type=jnp.float32).astype(jnp.bfloat16)

def by_head(matrix):
    return matrix.reshape(TOKENS, H, DH).transpose(1, 0, 2)

def one_head(inputs):
    query_slice, key_slice, value_slice, rate_slice, gate_w, down_w, up_w = inputs
    query_norm = norm_rows(query_slice)
    key_norm = norm_rows(key_slice)
    fast_f32 = (gate_w, down_w, up_w)
    pieces = []
    for group in range(2):
        lower = group * GROUP
        upper = lower + GROUP
        fast_bf = tuple((weight.astype(jnp.bfloat16) for weight in fast_f32))
        grad_terms = fast_terms(fast_bf, key_norm[lower:upper], value_slice[lower:upper], rate_slice[lower:upper])
        fast_f32 = tuple((rescale(weight, weight - summed) for weight, summed in zip(fast_f32, grad_terms)))
        renewed_bf = tuple((weight.astype(jnp.bfloat16) for weight in fast_f32))
        pieces.append(apply_fast(renewed_bf, query_norm[lower:upper]))
    return jnp.concatenate(pieces, axis=0)

def reference(queries, key_rows, value_rows, learn_rates, gate_fast, down_fast, up_fast):
    fast_heads = lax.map(one_head, (by_head(queries), by_head(key_rows), by_head(value_rows), learn_rates.T, gate_fast, down_fast, up_fast))
    fast_out = fast_heads.transpose(1, 0, 2).reshape(TOKENS, D)
    attn_heads = D // AH
    score_scale = 1.0 / math.sqrt(AH)
    pad_keys = jnp.concatenate([jnp.zeros((WINDOW, D), jnp.bfloat16), key_rows], axis=0)
    pad_values = jnp.concatenate([jnp.zeros((WINDOW, D), jnp.bfloat16), value_rows], axis=0)

    def one_block(block):
        start = block * WINDOW
        query_block = lax.dynamic_slice_in_dim(queries, start, WINDOW, 0).reshape(WINDOW, attn_heads, AH).astype(jnp.float32)
        key_block = lax.dynamic_slice_in_dim(pad_keys, start, 2 * WINDOW, 0).reshape(2 * WINDOW, attn_heads, AH).astype(jnp.float32)
        value_block = lax.dynamic_slice_in_dim(pad_values, start, 2 * WINDOW, 0).reshape(2 * WINDOW, attn_heads, AH).astype(jnp.float32)
        scores = jnp.einsum('qhd,khd->hqk', query_block, key_block) * score_scale
        query_pos = start + jnp.arange(WINDOW, dtype=jnp.int32)[:, None]
        key_pos = start - WINDOW + jnp.arange(2 * WINDOW, dtype=jnp.int32)[None, :]
        allowed = (key_pos <= query_pos) & (key_pos > query_pos - WINDOW) & (key_pos >= 0)
        scores = jnp.where(allowed[None], scores, jnp.float32(-1e+30))
        top_score = lax.optimization_barrier(jnp.max(scores, axis=-1, keepdims=True))
        expo = jnp.exp(scores - top_score)
        attend = (expo / lax.optimization_barrier(jnp.sum(expo, axis=-1, keepdims=True))).astype(jnp.bfloat16)
        return jnp.einsum('hqk,khd->qhd', attend.astype(jnp.float32), value_block).reshape(WINDOW, D)
    blocks = jnp.arange(TOKENS // WINDOW, dtype=jnp.int32)
    attended = lax.map(one_block, blocks).reshape(TOKENS, D)
    return (fast_out.astype(jnp.float32) + attended).astype(jnp.bfloat16)
```

```python
import functools
import math

import jax
import jax.numpy as jnp
from jax import lax
from jax.experimental import pallas as pl
from jax.experimental.pallas import tpu as pltpu
from jax.sharding import PartitionSpec as P

AH = 128
WINDOW = 512
TILE = 256
NZ = 8
NY = 4
EPSILON = 1e-06
MESH = pl.DeviceIdType.MESH
HOPS = ((4, 3), (3, 4), (4, 3))
F32 = jnp.float32
BF16 = jnp.bfloat16


def dot_nn(a, b):
    return lax.dot_general(a, b, (((1,), (0,)), ((), ())), preferred_element_type=F32)


def dot_nt(a, b):
    return lax.dot_general(a, b, (((1,), (1,)), ((), ())), preferred_element_type=F32)


def norm_rows(rows):
    as_float = rows.astype(F32)
    mean = jnp.mean(as_float * as_float, axis=-1, keepdims=True)
    return (as_float / jnp.sqrt(mean + EPSILON)).astype(BF16)


def kernel(
    q_hbm, k_hbm, v_hbm, rate_hbm, gate_hbm, down_hbm, up_hbm, out_hbm,
    q_ref, k_ref, v_ref, rate_ref, w0_ref, w0t_ref, kn_ref, wa_ref, wdn_ref, wb_ref, wc_ref,
    hid_ref, g_ref, rs_send, rs_recv, ysend, yrecv, up_recv, up_pair, att_ref, out_ref,
    load_sem, out_sem, halo_ssem, halo_rsem, rs_ssem, rs_rsem, y_ssem, y_rsem, up_ssem, up_rsem,
    pair_ssem, pair_rsem, aga_ssem, aga_rsem, agb_ssem, agb_rsem,
):
    rows, width = q_hbm.shape
    chunk = width // NZ
    head = lax.axis_index("head")
    seq = lax.axis_index("seq")
    y = seq // NZ
    z = seq % NZ
    upper = y >= NY // 2
    lower = y < NY // 2
    last = NZ * NY - 1
    z_next = y * NZ + lax.rem(z + 1, NZ)
    z_prev = y * NZ + lax.rem(z + NZ - 1, NZ)
    pair = (y + 1 - 2 * lax.rem(y, 2)) * NZ + z
    across = (NY - 1 - y) * NZ + z
    heads = width // AH
    tiles = rows // TILE

    def signal(target):
        pl.semaphore_signal(pltpu.get_barrier_semaphore(), inc=1, device_id=(head, target), device_id_type=MESH)

    def remote(src, dst, ssem, rsem, target):
        return pltpu.make_async_remote_copy(
            src_ref=src, dst_ref=dst, send_sem=ssem, recv_sem=rsem, device_id=(head, target), device_id_type=MESH
        )

    loads = [
        pltpu.make_async_copy(k_hbm, k_ref.at[pl.ds(WINDOW, rows)], load_sem.at[0]),
        pltpu.make_async_copy(gate_hbm.at[0], w0_ref.at[1], load_sem.at[1]),
        pltpu.make_async_copy(up_hbm.at[0], w0_ref.at[2], load_sem.at[2]),
        pltpu.make_async_copy(down_hbm.at[0], w0_ref.at[0], load_sem.at[3]),
        pltpu.make_async_copy(v_hbm, v_ref.at[pl.ds(WINDOW, rows)], load_sem.at[4]),
        pltpu.make_async_copy(rate_hbm, rate_ref, load_sem.at[5]),
        pltpu.make_async_copy(q_hbm, q_ref, load_sem.at[6]),
    ]
    for load in loads:
        load.start()

    for target in (z_next, z_prev, pair, across):
        signal(target)
    edge_next = jnp.logical_and(z == NZ - 1, y < NY - 1)
    edge_prev = jnp.logical_and(z == 0, y > 0)

    @pl.when(edge_next)
    def _():
        signal(seq + 1)

    @pl.when(edge_prev)
    def _():
        signal(seq - 1)

    for index, load in ((1, loads[1]), (2, loads[2]), (0, loads[3])):
        load.wait()
        w0t_ref[index] = w0_ref[index].T
    loads[0].wait()

    def norm_keys(tile, carry):
        at = pl.multiple_of(tile * TILE, TILE)
        kn_ref[pl.ds(at, TILE), :] = norm_rows(k_ref[pl.ds(at + WINDOW, TILE), :])
        return carry

    lax.fori_loop(0, tiles, norm_keys, 0)
    for load in loads[4:]:
        load.wait()

    pl.semaphore_wait(
        pltpu.get_barrier_semaphore(), 4 + edge_next.astype(jnp.int32) + edge_prev.astype(jnp.int32)
    )

    halo = [
        remote(
            ref.at[pl.ds(rows, WINDOW)], ref.at[pl.ds(0, WINDOW)], halo_ssem.at[i], halo_rsem.at[i],
            lax.rem(seq + 1, NZ * NY),
        )
        for i, ref in enumerate((k_ref, v_ref))
    ]

    @pl.when(seq == 0)
    def _():
        k_ref[pl.ds(0, WINDOW), :] = jnp.zeros((WINDOW, width), BF16)
        v_ref[pl.ds(0, WINDOW), :] = jnp.zeros((WINDOW, width), BF16)

    def attention_tile(tile, carry):
        at = pl.multiple_of(tile * TILE, TILE)
        row = lax.broadcasted_iota(jnp.int32, (TILE, TILE), 0)
        col = lax.broadcasted_iota(jnp.int32, (TILE, TILE), 1)
        recent = col <= row
        real0 = jnp.logical_or(seq > 0, at >= WINDOW)
        real1 = jnp.logical_or(seq > 0, at + TILE >= WINDOW)
        scale = math.log2(math.e) / math.sqrt(AH)
        for a in range(heads):
            lanes = slice(a * AH, (a + 1) * AH)
            q = q_ref[pl.ds(at, TILE), lanes]
            s0 = dot_nt(q, k_ref[pl.ds(at, TILE), lanes])
            s1 = dot_nt(q, k_ref[pl.ds(at + TILE, TILE), lanes])
            s2 = dot_nt(q, k_ref[pl.ds(at + 2 * TILE, TILE), lanes])
            edge = jnp.where(recent, s2, jnp.where(real0, s0, -1e30))
            middle = jnp.where(real1, s1, -1e30)
            top = jnp.max(jnp.maximum(edge, middle), axis=-1, keepdims=True)
            edge = jnp.exp2((edge - top) * scale)
            middle = jnp.exp2((middle - top) * scale)
            total = jnp.sum(edge + middle, axis=-1, keepdims=True)
            out = dot_nn(middle.astype(BF16), v_ref[pl.ds(at + TILE, TILE), lanes])
            out += dot_nn(jnp.where(recent, edge, 0.0).astype(BF16), v_ref[pl.ds(at + 2 * TILE, TILE), lanes])
            out += dot_nn(jnp.where(recent, 0.0, edge).astype(BF16), v_ref[pl.ds(at, TILE), lanes])
            att_ref[pl.ds(at, TILE), lanes] = out / total
        return carry

    def attention():
        inner = WINDOW // TILE
        lax.fori_loop(inner, tiles, attention_tile, 0)

        @pl.when(seq > 0)
        def _():
            for copy in halo:
                copy.wait_recv()

        lax.fori_loop(0, inner, attention_tile, 0)

    def update(index, old, step):
        moved = old + step
        before = jnp.sum(old * old, axis=-1, keepdims=True)
        after = jnp.sum(moved * moved, axis=-1, keepdims=True)
        return moved * (jnp.sqrt(before) / jnp.sqrt(after + EPSILON))

    def rows_of(position):
        return pl.ds(pl.multiple_of(lax.rem(position + 2 * NZ, NZ) * chunk, chunk), chunk)

    own = rows_of(z)
    signs = (1, -1)
    ring = (z_next, z_prev)

    def gather_send(ref, ssem, rsem, index, way, step):
        part = ref.at[index, rows_of(z - signs[way] * step)]
        return remote(part, part, ssem.at[index, way, step], rsem.at[index, way, step], ring[way])

    def gather_take(ref, ssem, rsem, index, way, step):
        part = ref.at[index, rows_of(z - signs[way] * (step + 1))]
        return remote(part, part, ssem.at[index, way, step], rsem.at[index, way, step], ring[way])

    def gather_rest(ref, ssem, rsem):
        for step in range(1, 5):
            for index in range(3):
                for way in range(2):
                    if step <= HOPS[index][way]:
                        gather_take(ref, ssem, rsem, index, way, step - 1).wait_recv()
                        if step < HOPS[index][way]:
                            gather_send(ref, ssem, rsem, index, way, step).start()

    def gather_drain(ref, ssem, rsem):
        for index in range(3):
            for way in range(2):
                for step in range(HOPS[index][way]):
                    gather_send(ref, ssem, rsem, index, way, step).wait_send()

    up_copies = [remote(ysend.at[i], up_recv.at[i], up_ssem.at[i], up_rsem.at[i], across) for i in range(3)]
    pair_copies = [remote(up_recv.at[i], up_pair.at[i], pair_ssem.at[i], pair_rsem.at[i], pair) for i in range(3)]
    y_copies = [remote(ysend.at[i], yrecv.at[i], y_ssem.at[i], y_rsem.at[i], pair) for i in range(3)]

    @pl.when(jnp.logical_and(seq >= NZ * NY // 2 - 1, seq < last))
    def _():
        for copy in halo:
            copy.start()

    @pl.when(lower)
    def _():
        wa_ref[1] = w0t_ref[1].astype(BF16)
        wa_ref[2] = w0t_ref[2].astype(BF16)
        wdn_ref[...] = w0_ref[0].astype(BF16)
        for index in range(3):
            wc_ref[index] = w0t_ref[index, own, :]

    @pl.when(upper)
    def _():
        attention()
        for index in range(3):
            up_copies[index].wait_recv()
            pair_copies[index].start()
        for index in range(3):
            pair_copies[index].wait_recv()
            step = up_recv[index].astype(F32) + up_pair[index].astype(F32)
            fresh = update(index, w0t_ref[index, own, :], step)
            wc_ref[index] = fresh
            wa_ref[index, own, :] = fresh.astype(BF16)
            for way in range(2):
                gather_send(wa_ref, aga_ssem, aga_rsem, index, way, 0).start()
        gather_rest(wa_ref, aga_ssem, aga_rsem)
        gather_drain(wa_ref, aga_ssem, aga_rsem)
        for index in range(3):
            pair_copies[index].wait_send()
        wdn_ref[...] = wa_ref[0].T

    def grad_tile(tile, carry):
        at = pl.multiple_of(tile * TILE, TILE)
        keys = kn_ref[pl.ds(at, TILE), :]
        gate_pre = dot_nt(wa_ref[1], keys)
        up_pre = dot_nt(wa_ref[2], keys)
        rate = rate_ref[0:1, pl.ds(at, TILE)].astype(F32)
        grad = dot_nt(wdn_ref[...], v_ref[pl.ds(at + WINDOW, TILE), :]) * rate
        sig = jax.nn.sigmoid(gate_pre)
        act = gate_pre * sig
        hid_ref[0, :, pl.ds(at, TILE)] = (act * up_pre * rate).astype(BF16)
        hid_ref[1, :, pl.ds(at, TILE)] = (grad * up_pre * sig * (1.0 + gate_pre * (1.0 - sig))).astype(BF16)
        hid_ref[2, :, pl.ds(at, TILE)] = (grad * act).astype(BF16)
        return carry

    lax.fori_loop(0, tiles, grad_tile, 0)

    def rs_copy(index, way, step):
        return remote(
            rs_send.at[index, way, step], rs_recv.at[index, way, step],
            rs_ssem.at[index, way, step], rs_rsem.at[index, way, step], ring[way],
        )

    def scatter_step(index, way, step):
        hops = HOPS[index][way]
        if step >= hops:
            return
        value = g_ref[index, rows_of(z + signs[way] * (hops - step)), :]
        if step > 0:
            rs_copy(index, way, step - 1).wait_recv()
            value = value + rs_recv[index, way, step - 1].astype(F32)
        rs_send[index, way, step] = value.astype(BF16)
        rs_copy(index, way, step).start()

    g_ref[0] = dot_nn(hid_ref[0], v_ref[pl.ds(WINDOW, rows), :]).T
    scatter_step(0, 0, 0)
    scatter_step(0, 1, 0)
    g_ref[1] = dot_nn(hid_ref[1], kn_ref[...])
    scatter_step(1, 0, 0)
    scatter_step(1, 1, 0)
    g_ref[2] = dot_nn(hid_ref[2], kn_ref[...])
    scatter_step(2, 0, 0)
    scatter_step(2, 1, 0)
    for step in range(1, 4):
        for index in range(3):
            for way in range(2):
                scatter_step(index, way, step)
    for index in range(3):
        value = g_ref[index, own, :]
        for way in range(2):
            final = HOPS[index][way] - 1
            rs_copy(index, way, final).wait_recv()
            value = value + rs_recv[index, way, final].astype(F32)
        ysend[index] = value.astype(BF16)
        y_copies[index].start()

        @pl.when(lower)
        def _():
            up_copies[index].start()

    @pl.when(seq < NZ * NY // 2 - 1)
    def _():
        for copy in halo:
            copy.start()

    for index in range(3):
        y_copies[index].wait_recv()
        step = ysend[index].astype(F32) + yrecv[index].astype(F32)
        wb_ref[index, own, :] = update(index, wc_ref[index], step).astype(BF16)
        for way in range(2):
            gather_send(wb_ref, agb_ssem, agb_rsem, index, way, 0).start()
    gather_rest(wb_ref, agb_ssem, agb_rsem)

    @pl.when(lower)
    def _():
        attention()

    out_copies = []

    def apply_tile(tile, carry):
        at = pl.multiple_of(tile * TILE, TILE)
        queries = norm_rows(q_ref[pl.ds(at, TILE), :])
        gate_pre = dot_nt(queries, wb_ref[1])
        up_pre = dot_nt(queries, wb_ref[2])
        hidden = (gate_pre * jax.nn.sigmoid(gate_pre) * up_pre).astype(BF16)
        fast = dot_nt(hidden, wb_ref[0]).astype(BF16)
        out_ref[pl.ds(at, TILE), :] = (fast.astype(F32) + att_ref[pl.ds(at, TILE), :]).astype(BF16)
        pltpu.make_async_copy(
            out_ref.at[pl.ds(at, TILE)], out_hbm.at[pl.ds(at, TILE)], out_sem.at[tile]
        ).start()
        return carry

    lax.fori_loop(0, tiles, apply_tile, 0)

    gather_drain(wb_ref, agb_ssem, agb_rsem)
    for index in range(3):
        for way in range(2):
            for step in range(HOPS[index][way]):
                rs_copy(index, way, step).wait_send()
        y_copies[index].wait_send()

    @pl.when(lower)
    def _():
        for index in range(3):
            up_copies[index].wait_send()

    @pl.when(seq < last)
    def _():
        for copy in halo:
            copy.wait_send()

    for tile in range(tiles):
        at = tile * TILE
        pltpu.make_async_copy(
            out_ref.at[pl.ds(at, TILE)], out_hbm.at[pl.ds(at, TILE)], out_sem.at[tile]
        ).wait()


def on_device(queries, key_rows, value_rows, learn_rates, gate_fast, down_fast, up_fast):
    rows, width = queries.shape
    chunk = width // NZ
    tiles = rows // TILE
    dma = pltpu.SemaphoreType.DMA
    square = (3, width, width)
    parts = (3, 2, 4, chunk, width)
    return pl.pallas_call(
        kernel,
        name="layer",
        out_shape=jax.ShapeDtypeStruct((rows, width), BF16),
        in_specs=[pl.BlockSpec(memory_space=pl.ANY)] * 7,
        out_specs=pl.BlockSpec(memory_space=pl.ANY),
        scratch_shapes=[
            pltpu.VMEM((rows, width), BF16),
            pltpu.VMEM((WINDOW + rows, width), BF16),
            pltpu.VMEM((WINDOW + rows, width), BF16),
            pltpu.VMEM((1, rows), BF16),
            pltpu.VMEM(square, F32),
            pltpu.VMEM(square, F32),
            pltpu.VMEM((rows, width), BF16),
            pltpu.VMEM(square, BF16),
            pltpu.VMEM(square[1:], BF16),
            pltpu.VMEM(square, BF16),
            pltpu.VMEM((3, chunk, width), F32),
            pltpu.VMEM((3, width, rows), BF16),
            pltpu.VMEM(square, F32),
            pltpu.VMEM(parts, BF16),
            pltpu.VMEM(parts, BF16),
            pltpu.VMEM((3, chunk, width), BF16),
            pltpu.VMEM((3, chunk, width), BF16),
            pltpu.VMEM((3, chunk, width), BF16),
            pltpu.VMEM((3, chunk, width), BF16),
            pltpu.VMEM((rows, width), F32),
            pltpu.VMEM((rows, width), BF16),
            dma((7,)),
            dma((tiles,)),
            dma((2,)),
            dma((2,)),
            dma((3, 2, 4)),
            dma((3, 2, 4)),
            dma((3,)),
            dma((3,)),
            dma((3,)),
            dma((3,)),
            dma((3,)),
            dma((3,)),
            dma((3, 2, 4)),
            dma((3, 2, 4)),
            dma((3, 2, 4)),
            dma((3, 2, 4)),
        ],
        compiler_params=pltpu.CompilerParams(
            collective_id=0, has_side_effects=True, vmem_limit_bytes=60 * 1024 * 1024
        ),
    )(queries, key_rows, value_rows, learn_rates.T, gate_fast, down_fast, up_fast)


def solution(mesh):
    return jax.shard_map(
        on_device,
        mesh=mesh,
        in_specs=(
            P("seq", "head"),
            P("seq", "head"),
            P("seq", "head"),
            P("seq", "head"),
            P("head", None, None),
            P("head", None, None),
            P("head", None, None),
        ),
        out_specs=P("seq", "head"),
        check_vma=False,
    )
```

```python
import functools
import math

import jax
import jax.numpy as jnp
from jax import lax
from jax.experimental import pallas as pl
from jax.experimental.pallas import tpu as pltpu
from jax.sharding import PartitionSpec as P

AH = 128
WINDOW = 512
TILE = 256
NZ = 8
NY = 4
EPSILON = 1e-06
MESH = pl.DeviceIdType.MESH
SPLIT = 2
PIECES = tuple((index, part) for index in range(3) for part in range(SPLIT))


def hops_of(part, way):
    return 4 - (part + way) % 2


F32 = jnp.float32
BF16 = jnp.bfloat16


def dot_nn(a, b):
    return lax.dot_general(a, b, (((1,), (0,)), ((), ())), preferred_element_type=F32)


def dot_nt(a, b):
    return lax.dot_general(a, b, (((1,), (1,)), ((), ())), preferred_element_type=F32)


def norm_rows(rows):
    as_float = rows.astype(F32)
    mean = jnp.mean(as_float * as_float, axis=-1, keepdims=True)
    return (as_float / jnp.sqrt(mean + EPSILON)).astype(BF16)


def kernel(
    q_hbm, k_hbm, v_hbm, rate_hbm, gate_hbm, down_hbm, up_hbm, out_hbm,
    q_ref, k_ref, v_ref, rate_ref, w0_ref, w0t_ref, kn_ref, wa_ref, wdn_ref, wb_ref, wc_ref,
    hid_ref, g_ref, rs_send, rs_recv, ysend, yrecv, up_recv, up_pair, att_ref, out_ref,
    load_sem, out_sem, halo_ssem, halo_rsem, rs_ssem, rs_rsem, y_ssem, y_rsem, up_ssem, up_rsem,
    pair_ssem, pair_rsem, aga_ssem, aga_rsem, agb_ssem, agb_rsem,
):
    rows, width = q_hbm.shape
    chunk = width // NZ
    piece = chunk // SPLIT
    head = lax.axis_index("head")
    seq = lax.axis_index("seq")
    y = seq // NZ
    z = seq % NZ
    upper = y >= NY // 2
    lower = y < NY // 2
    last = NZ * NY - 1
    z_next = y * NZ + lax.rem(z + 1, NZ)
    z_prev = y * NZ + lax.rem(z + NZ - 1, NZ)
    pair = (y + 1 - 2 * lax.rem(y, 2)) * NZ + z
    across = (NY - 1 - y) * NZ + z
    heads = width // AH
    tiles = rows // TILE

    def signal(target):
        pl.semaphore_signal(pltpu.get_barrier_semaphore(), inc=1, device_id=(head, target), device_id_type=MESH)

    def remote(src, dst, ssem, rsem, target):
        return pltpu.make_async_remote_copy(
            src_ref=src, dst_ref=dst, send_sem=ssem, recv_sem=rsem, device_id=(head, target), device_id_type=MESH
        )

    loads = [
        pltpu.make_async_copy(k_hbm, k_ref.at[pl.ds(WINDOW, rows)], load_sem.at[0]),
        pltpu.make_async_copy(gate_hbm.at[0], w0_ref.at[1], load_sem.at[1]),
        pltpu.make_async_copy(up_hbm.at[0], w0_ref.at[2], load_sem.at[2]),
        pltpu.make_async_copy(down_hbm.at[0], w0_ref.at[0], load_sem.at[3]),
        pltpu.make_async_copy(v_hbm, v_ref.at[pl.ds(WINDOW, rows)], load_sem.at[4]),
        pltpu.make_async_copy(rate_hbm, rate_ref, load_sem.at[5]),
        pltpu.make_async_copy(q_hbm, q_ref, load_sem.at[6]),
    ]
    for load in (loads[0], loads[1], loads[2], loads[4], loads[5], loads[3]):
        load.start()

    for target in (z_next, z_prev, pair, across):
        signal(target)
    edge_next = jnp.logical_and(z == NZ - 1, y < NY - 1)
    edge_prev = jnp.logical_and(z == 0, y > 0)

    @pl.when(edge_next)
    def _():
        signal(seq + 1)

    @pl.when(edge_prev)
    def _():
        signal(seq - 1)

    def norm_keys(tile, carry):
        at = pl.multiple_of(tile * TILE, TILE)
        kn_ref[pl.ds(at, TILE), :] = norm_rows(k_ref[pl.ds(at + WINDOW, TILE), :])
        return carry

    loads[0].wait()
    lax.fori_loop(0, tiles, norm_keys, 0)
    for index, load in ((1, loads[1]), (2, loads[2]), (0, loads[3])):
        load.wait()
        w0t_ref[index] = w0_ref[index].T
    loads[6].start()
    loads[4].wait()
    loads[5].wait()

    pl.semaphore_wait(
        pltpu.get_barrier_semaphore(), 4 + edge_next.astype(jnp.int32) + edge_prev.astype(jnp.int32)
    )

    halo = [
        remote(
            ref.at[pl.ds(rows, WINDOW)], ref.at[pl.ds(0, WINDOW)], halo_ssem.at[i], halo_rsem.at[i],
            lax.rem(seq + 1, NZ * NY),
        )
        for i, ref in enumerate((k_ref, v_ref))
    ]

    @pl.when(seq == 0)
    def _():
        k_ref[pl.ds(0, WINDOW), :] = jnp.zeros((WINDOW, width), BF16)
        v_ref[pl.ds(0, WINDOW), :] = jnp.zeros((WINDOW, width), BF16)

    def attend(tile, a):
        at = pl.multiple_of(tile * TILE, TILE)
        row = lax.broadcasted_iota(jnp.int32, (TILE, TILE), 0)
        col = lax.broadcasted_iota(jnp.int32, (TILE, TILE), 1)
        recent = col <= row
        real0 = jnp.logical_or(seq > 0, at >= WINDOW)
        real1 = jnp.logical_or(seq > 0, at + TILE >= WINDOW)
        scale = math.log2(math.e) / math.sqrt(AH)
        lanes = slice(a * AH, (a + 1) * AH)
        q = q_ref[pl.ds(at, TILE), lanes]
        s0 = dot_nt(q, k_ref[pl.ds(at, TILE), lanes])
        s1 = dot_nt(q, k_ref[pl.ds(at + TILE, TILE), lanes])
        s2 = dot_nt(q, k_ref[pl.ds(at + 2 * TILE, TILE), lanes])
        edge = jnp.where(recent, s2, jnp.where(real0, s0, -1e30))
        middle = jnp.where(real1, s1, -1e30)
        top = jnp.max(jnp.maximum(edge, middle), axis=-1, keepdims=True)
        edge = jnp.exp2((edge - top) * scale)
        middle = jnp.exp2((middle - top) * scale)
        total = jnp.sum(edge + middle, axis=-1, keepdims=True)
        out = dot_nn(middle.astype(BF16), v_ref[pl.ds(at + TILE, TILE), lanes])
        out += dot_nn(jnp.where(recent, edge, 0.0).astype(BF16), v_ref[pl.ds(at + 2 * TILE, TILE), lanes])
        out += dot_nn(jnp.where(recent, 0.0, edge).astype(BF16), v_ref[pl.ds(at, TILE), lanes])
        att_ref[pl.ds(at, TILE), lanes] = out / total

    def attend_tile(tile, carry):
        for a in range(heads):
            attend(tile, a)
        return carry

    inner = WINDOW // TILE

    def attend_own():
        lax.fori_loop(inner, tiles, attend_tile, 0)

    def halo_ready():
        for copy in halo:
            copy.wait_recv()

    def update(old, step):
        moved = old + step
        before = jnp.sum(old * old, axis=-1, keepdims=True)
        after = jnp.sum(moved * moved, axis=-1, keepdims=True)
        return moved * (jnp.sqrt(before) / jnp.sqrt(after + EPSILON))

    def rows_of(position, part):
        return pl.ds(pl.multiple_of(lax.rem(position + 2 * NZ, NZ) * chunk + part * piece, piece), piece)

    own = pl.ds(pl.multiple_of(z * chunk, chunk), chunk)
    signs = (1, -1)
    ring = (z_next, z_prev)

    def gather_send(ref, ssem, rsem, index, part, way, step):
        block = ref.at[index, rows_of(z - signs[way] * step, part)]
        return remote(block, block, ssem.at[index, part, way, step], rsem.at[index, part, way, step], ring[way])

    def gather_take(ref, ssem, rsem, index, part, way, step):
        block = ref.at[index, rows_of(z - signs[way] * (step + 1), part)]
        return remote(block, block, ssem.at[index, part, way, step], rsem.at[index, part, way, step], ring[way])

    def gather_rest(ref, ssem, rsem, fill=None):
        for step in range(1, 5):
            for index, part in PIECES:
                for way in range(2):
                    if step <= hops_of(part, way):
                        gather_take(ref, ssem, rsem, index, part, way, step - 1).wait_recv()
                        if step < hops_of(part, way):
                            gather_send(ref, ssem, rsem, index, part, way, step).start()
                if fill is not None and (index, part) in PIECES[len(PIECES) // 2 - 1 :: len(PIECES) // 2]:
                    fill()

    def gather_drain(ref, ssem, rsem):
        for index, part in PIECES:
            for way in range(2):
                for step in range(hops_of(part, way)):
                    gather_send(ref, ssem, rsem, index, part, way, step).wait_send()

    def along_y(src, dst, ssem, rsem, target):
        return {(i, p): remote(src.at[i, p], dst.at[i, p], ssem.at[i, p], rsem.at[i, p], target) for i, p in PIECES}

    up_copies = along_y(ysend, up_recv, up_ssem, up_rsem, across)
    pair_copies = along_y(up_recv, up_pair, pair_ssem, pair_rsem, pair)
    y_copies = along_y(ysend, yrecv, y_ssem, y_rsem, pair)

    @pl.when(jnp.logical_and(upper, seq < last))
    def _():
        for copy in halo:
            copy.start()

    @pl.when(lower)
    def _():
        wa_ref[1] = w0t_ref[1].astype(BF16)
        wa_ref[2] = w0t_ref[2].astype(BF16)
        wdn_ref[...] = w0_ref[0].astype(BF16)
        for index in range(3):
            wc_ref[index] = w0t_ref[index, own, :]

    loads[6].wait()

    @pl.when(upper)
    def _():
        attend_own()
        for at in PIECES:
            up_copies[at].wait_recv()
            pair_copies[at].start()
        for index, part in PIECES:
            pair_copies[index, part].wait_recv()
            step = up_recv[index, part].astype(F32) + up_pair[index, part].astype(F32)
            fresh = update(w0t_ref[index, rows_of(z, part), :], step)
            wc_ref[index, pl.ds(part * piece, piece), :] = fresh
            wa_ref[index, rows_of(z, part), :] = fresh.astype(BF16)
            for way in range(2):
                gather_send(wa_ref, aga_ssem, aga_rsem, index, part, way, 0).start()
        gather_rest(wa_ref, aga_ssem, aga_rsem)
        gather_drain(wa_ref, aga_ssem, aga_rsem)
        for at in PIECES:
            pair_copies[at].wait_send()
        wdn_ref[...] = wa_ref[0].T

    def grad_tile(tile, carry):
        at = pl.multiple_of(tile * TILE, TILE)
        keys = kn_ref[pl.ds(at, TILE), :]
        gate_pre = dot_nt(wa_ref[1], keys)
        up_pre = dot_nt(wa_ref[2], keys)
        rate = rate_ref[0:1, pl.ds(at, TILE)].astype(F32)
        grad = dot_nt(wdn_ref[...], v_ref[pl.ds(at + WINDOW, TILE), :]) * rate
        sig = jax.nn.sigmoid(gate_pre)
        act = gate_pre * sig
        hid_ref[0, :, pl.ds(at, TILE)] = (act * up_pre * rate).astype(BF16)
        hid_ref[1, :, pl.ds(at, TILE)] = (grad * up_pre * sig * (1.0 + gate_pre * (1.0 - sig))).astype(BF16)
        hid_ref[2, :, pl.ds(at, TILE)] = (grad * act).astype(BF16)
        return carry

    lax.fori_loop(0, tiles, grad_tile, 0)

    def rs_copy(index, part, way, step):
        at = (index, part, way, step)
        return remote(rs_send.at[at], rs_recv.at[at], rs_ssem.at[at], rs_rsem.at[at], ring[way])

    def scatter_step(index, part, way, step):
        hops = hops_of(part, way)
        if step >= hops:
            return
        value = g_ref[index, rows_of(z + signs[way] * (hops - step), part), :]
        if step > 0:
            rs_copy(index, part, way, step - 1).wait_recv()
            value = value + rs_recv[index, part, way, step - 1].astype(F32)
        rs_send[index, part, way, step] = value.astype(BF16)
        rs_copy(index, part, way, step).start()

    def scatter_first(index):
        for part in range(SPLIT):
            for way in range(2):
                scatter_step(index, part, way, 0)

    g_ref[0] = dot_nn(hid_ref[0], v_ref[pl.ds(WINDOW, rows), :]).T
    scatter_first(0)
    g_ref[1] = dot_nn(hid_ref[1], kn_ref[...])
    scatter_first(1)
    g_ref[2] = dot_nn(hid_ref[2], kn_ref[...])
    scatter_first(2)
    for step in range(1, 4):
        for index, part in PIECES:
            for way in range(2):
                scatter_step(index, part, way, step)
    for index, part in PIECES:
        value = g_ref[index, rows_of(z, part), :]
        for way in range(2):
            final = hops_of(part, way) - 1
            rs_copy(index, part, way, final).wait_recv()
            value = value + rs_recv[index, part, way, final].astype(F32)
        ysend[index, part] = value.astype(BF16)
        y_copies[index, part].start()

        @pl.when(lower)
        def _():
            up_copies[index, part].start()

    for index, part in PIECES:
        y_copies[index, part].wait_recv()
        step = ysend[index, part].astype(F32) + yrecv[index, part].astype(F32)
        old = wc_ref[index, pl.ds(part * piece, piece), :]
        wb_ref[index, rows_of(z, part), :] = update(old, step).astype(BF16)
        for way in range(2):
            gather_send(wb_ref, agb_ssem, agb_rsem, index, part, way, 0).start()

    @pl.when(lower)
    def _():
        for at in PIECES:
            up_copies[at].wait_send()
        for copy in halo:
            copy.start()

    @pl.when(upper)
    def _():
        halo_ready()

    slots = [(tile, a) for tile in range(inner) for a in range(heads)]

    def fill():
        if slots:
            tile, a = slots.pop(0)

            @pl.when(upper)
            def _():
                attend(tile, a)

    gather_rest(wb_ref, agb_ssem, agb_rsem, fill)
    while slots:
        fill()

    @pl.when(lower)
    def _():
        attend_own()

        @pl.when(seq > 0)
        def _():
            halo_ready()

        lax.fori_loop(0, inner, attend_tile, 0)

    out_copies = []

    def apply_tile(tile, carry):
        at = pl.multiple_of(tile * TILE, TILE)
        queries = norm_rows(q_ref[pl.ds(at, TILE), :])
        gate_pre = dot_nt(queries, wb_ref[1])
        up_pre = dot_nt(queries, wb_ref[2])
        hidden = (gate_pre * jax.nn.sigmoid(gate_pre) * up_pre).astype(BF16)
        fast = dot_nt(hidden, wb_ref[0]).astype(BF16)
        out_ref[pl.ds(at, TILE), :] = (fast.astype(F32) + att_ref[pl.ds(at, TILE), :]).astype(BF16)
        pltpu.make_async_copy(
            out_ref.at[pl.ds(at, TILE)], out_hbm.at[pl.ds(at, TILE)], out_sem.at[tile]
        ).start()
        return carry

    lax.fori_loop(0, tiles, apply_tile, 0)

    gather_drain(wb_ref, agb_ssem, agb_rsem)
    for index, part in PIECES:
        for way in range(2):
            for step in range(hops_of(part, way)):
                rs_copy(index, part, way, step).wait_send()
        y_copies[index, part].wait_send()

    @pl.when(seq < last)
    def _():
        for copy in halo:
            copy.wait_send()

    for tile in range(tiles):
        at = tile * TILE
        pltpu.make_async_copy(
            out_ref.at[pl.ds(at, TILE)], out_hbm.at[pl.ds(at, TILE)], out_sem.at[tile]
        ).wait()


def on_device(queries, key_rows, value_rows, learn_rates, gate_fast, down_fast, up_fast):
    rows, width = queries.shape
    chunk = width // NZ
    tiles = rows // TILE
    dma = pltpu.SemaphoreType.DMA
    square = (3, width, width)
    piece = chunk // SPLIT
    parts = (3, SPLIT, 2, 4, piece, width)
    sems = (3, SPLIT, 2, 4)
    return pl.pallas_call(
        kernel,
        name="layer",
        out_shape=jax.ShapeDtypeStruct((rows, width), BF16),
        in_specs=[pl.BlockSpec(memory_space=pl.ANY)] * 7,
        out_specs=pl.BlockSpec(memory_space=pl.ANY),
        scratch_shapes=[
            pltpu.VMEM((rows, width), BF16),
            pltpu.VMEM((WINDOW + rows, width), BF16),
            pltpu.VMEM((WINDOW + rows, width), BF16),
            pltpu.VMEM((1, rows), BF16),
            pltpu.VMEM(square, F32),
            pltpu.VMEM(square, F32),
            pltpu.VMEM((rows, width), BF16),
            pltpu.VMEM(square, BF16),
            pltpu.VMEM(square[1:], BF16),
            pltpu.VMEM(square, BF16),
            pltpu.VMEM((3, chunk, width), F32),
            pltpu.VMEM((3, width, rows), BF16),
            pltpu.VMEM(square, F32),
            pltpu.VMEM(parts, BF16),
            pltpu.VMEM(parts, BF16),
            pltpu.VMEM((3, SPLIT, piece, width), BF16),
            pltpu.VMEM((3, SPLIT, piece, width), BF16),
            pltpu.VMEM((3, SPLIT, piece, width), BF16),
            pltpu.VMEM((3, SPLIT, piece, width), BF16),
            pltpu.VMEM((rows, width), F32),
            pltpu.VMEM((rows, width), BF16),
            dma((7,)),
            dma((tiles,)),
            dma((2,)),
            dma((2,)),
            dma(sems),
            dma(sems),
            dma((3, SPLIT)),
            dma((3, SPLIT)),
            dma((3, SPLIT)),
            dma((3, SPLIT)),
            dma((3, SPLIT)),
            dma((3, SPLIT)),
            dma(sems),
            dma(sems),
            dma(sems),
            dma(sems),
        ],
        compiler_params=pltpu.CompilerParams(
            collective_id=0, has_side_effects=True, vmem_limit_bytes=60 * 1024 * 1024
        ),
    )(queries, key_rows, value_rows, learn_rates.T, gate_fast, down_fast, up_fast)


def solution(mesh):
    return jax.shard_map(
        on_device,
        mesh=mesh,
        in_specs=(
            P("seq", "head"),
            P("seq", "head"),
            P("seq", "head"),
            P("seq", "head"),
            P("head", None, None),
            P("head", None, None),
            P("head", None, None),
        ),
        out_specs=P("seq", "head"),
        check_vma=False,
    )
```

```python
import functools
import math

import jax
import jax.numpy as jnp
from jax import lax
from jax.experimental import pallas as pl
from jax.experimental.pallas import tpu as pltpu
from jax.sharding import PartitionSpec as P

AH = 128
WINDOW = 512
TILE = 256
NZ = 8
NY = 4
EPSILON = 1e-06
MESH = pl.DeviceIdType.MESH
HOPS = ((4, 3), (3, 4))
FAR = (1, 1)
F32 = jnp.float32
BF16 = jnp.bfloat16


def dot_nn(a, b):
    return lax.dot_general(a, b, (((1,), (0,)), ((), ())), preferred_element_type=F32)


def dot_nt(a, b):
    return lax.dot_general(a, b, (((1,), (1,)), ((), ())), preferred_element_type=F32)


def norm_rows(rows):
    as_float = rows.astype(F32)
    mean = jnp.mean(as_float * as_float, axis=-1, keepdims=True)
    return (as_float / jnp.sqrt(mean + EPSILON)).astype(BF16)


def kernel(
    q_hbm, k_hbm, v_hbm, rate_hbm, gate_hbm, down_hbm, up_hbm, out_ref,
    q_ref, k_ref, v_ref, rate_ref, w0_ref, w0t_ref, kn_ref, wa_ref, wdn_ref, wb_ref, wc_ref,
    hid_ref, g_ref, rs_send, rs_recv, xs_send, xs_recv, up_send, up_recv, att_ref,
    load_sem, halo_ssem, halo_rsem, rs_ssem, rs_rsem, xs_ssem, xs_rsem, up_ssem, up_rsem,
    aga_ssem, aga_rsem, xa_ssem, xa_rsem, agb_ssem, agb_rsem, xb_ssem, xb_rsem,
):
    rows, width = q_hbm.shape
    chunk = width // NZ
    piece = chunk // 2
    head = lax.axis_index("head")
    seq = lax.axis_index("seq")
    y = seq // NZ
    z = seq % NZ
    upper = y >= NY // 2
    lower = y < NY // 2
    last = NZ * NY - 1
    z_next = y * NZ + lax.rem(z + 1, NZ)
    z_prev = y * NZ + lax.rem(z + NZ - 1, NZ)
    pair = (y + 1 - 2 * lax.rem(y, 2)) * NZ + z
    across = (NY - 1 - y) * NZ + z
    heads = width // AH
    home = jnp.minimum(lax.rem(y, 3), 1)
    part_of = (home, 1 - home)
    tiles = rows // TILE

    def signal(target):
        pl.semaphore_signal(pltpu.get_barrier_semaphore(), inc=1, device_id=(head, target), device_id_type=MESH)

    def remote(src, dst, ssem, rsem, target):
        return pltpu.make_async_remote_copy(
            src_ref=src, dst_ref=dst, send_sem=ssem, recv_sem=rsem, device_id=(head, target), device_id_type=MESH
        )

    loads = [
        pltpu.make_async_copy(k_hbm, k_ref.at[pl.ds(WINDOW, rows)], load_sem.at[0]),
        pltpu.make_async_copy(gate_hbm.at[0], w0_ref.at[1], load_sem.at[1]),
        pltpu.make_async_copy(up_hbm.at[0], w0_ref.at[2], load_sem.at[2]),
        pltpu.make_async_copy(down_hbm.at[0], w0_ref.at[0], load_sem.at[3]),
        pltpu.make_async_copy(v_hbm, v_ref.at[pl.ds(WINDOW, rows)], load_sem.at[4]),
        pltpu.make_async_copy(rate_hbm, rate_ref, load_sem.at[5]),
        pltpu.make_async_copy(q_hbm, q_ref, load_sem.at[6]),
    ]
    for load in (loads[0], loads[1], loads[2], loads[4], loads[5], loads[3]):
        load.start()

    far_next = y * NZ + lax.rem(z + 2, NZ)
    far_prev = y * NZ + lax.rem(z + NZ - 2, NZ)
    for target in (z_next, z_prev, far_next, far_prev, pair, across):
        signal(target)
    edge_next = jnp.logical_and(z == NZ - 1, y < NY - 1)
    edge_prev = jnp.logical_and(z == 0, y > 0)

    @pl.when(edge_next)
    def _():
        signal(seq + 1)

    @pl.when(edge_prev)
    def _():
        signal(seq - 1)

    def norm_keys(tile, carry):
        at = pl.multiple_of(tile * TILE, TILE)
        kn_ref[pl.ds(at, TILE), :] = norm_rows(k_ref[pl.ds(at + WINDOW, TILE), :])
        return carry

    loads[0].wait()
    lax.fori_loop(0, tiles, norm_keys, 0)
    for index, load in ((1, loads[1]), (2, loads[2]), (0, loads[3])):
        load.wait()
        w0t_ref[index] = w0_ref[index].T
    loads[6].start()
    loads[4].wait()
    loads[5].wait()

    pl.semaphore_wait(
        pltpu.get_barrier_semaphore(), 6 + edge_next.astype(jnp.int32) + edge_prev.astype(jnp.int32)
    )

    halo = [
        remote(
            ref.at[pl.ds(rows, WINDOW)], ref.at[pl.ds(0, WINDOW)], halo_ssem.at[i], halo_rsem.at[i],
            lax.rem(seq + 1, NZ * NY),
        )
        for i, ref in enumerate((k_ref, v_ref))
    ]

    @pl.when(seq == 0)
    def _():
        k_ref[pl.ds(0, WINDOW), :] = jnp.zeros((WINDOW, width), BF16)
        v_ref[pl.ds(0, WINDOW), :] = jnp.zeros((WINDOW, width), BF16)

    def attend(tile, a):
        at = pl.multiple_of(tile * TILE, TILE)
        row = lax.broadcasted_iota(jnp.int32, (TILE, TILE), 0)
        col = lax.broadcasted_iota(jnp.int32, (TILE, TILE), 1)
        recent = col <= row
        real0 = jnp.logical_or(seq > 0, at >= WINDOW)
        real1 = jnp.logical_or(seq > 0, at + TILE >= WINDOW)
        scale = math.log2(math.e) / math.sqrt(AH)
        lanes = slice(a * AH, (a + 1) * AH)
        q = q_ref[pl.ds(at, TILE), lanes]
        s0 = dot_nt(q, k_ref[pl.ds(at, TILE), lanes])
        s1 = dot_nt(q, k_ref[pl.ds(at + TILE, TILE), lanes])
        s2 = dot_nt(q, k_ref[pl.ds(at + 2 * TILE, TILE), lanes])
        edge = jnp.where(recent, s2, jnp.where(real0, s0, -1e30))
        middle = jnp.where(real1, s1, -1e30)
        top = jnp.max(jnp.maximum(edge, middle), axis=-1, keepdims=True)
        edge = jnp.exp2((edge - top) * scale)
        middle = jnp.exp2((middle - top) * scale)
        total = jnp.sum(edge + middle, axis=-1, keepdims=True)
        out = dot_nn(middle.astype(BF16), v_ref[pl.ds(at + TILE, TILE), lanes])
        out += dot_nn(jnp.where(recent, edge, 0.0).astype(BF16), v_ref[pl.ds(at + 2 * TILE, TILE), lanes])
        out += dot_nn(jnp.where(recent, 0.0, edge).astype(BF16), v_ref[pl.ds(at, TILE), lanes])
        att_ref[pl.ds(at, TILE), lanes] = out / total

    def attend_tile(tile, carry):
        for a in range(heads):
            attend(tile, a)
        return carry

    inner = WINDOW // TILE

    def attend_own():
        lax.fori_loop(inner, tiles, attend_tile, 0)

    def halo_ready():
        for copy in halo:
            copy.wait_recv()

    def update(old, step):
        moved = old + step
        before = jnp.sum(old * old, axis=-1, keepdims=True)
        after = jnp.sum(moved * moved, axis=-1, keepdims=True)
        return moved * (jnp.sqrt(before) / jnp.sqrt(after + EPSILON))

    def rows_of(position, role):
        start = lax.rem(position + 2 * NZ, NZ) * chunk + part_of[role] * piece
        return pl.ds(pl.multiple_of(start, piece), piece)

    def sign_of(index, way):
        return 1 if (way + index) % 2 == 0 else -1

    def near(index, way):
        return z_next if sign_of(index, way) > 0 else z_prev

    def far(index, way):
        return far_next if sign_of(index, way) > 0 else far_prev

    def gather_copy(gather, index, role, way, step, distance, target):
        ref, ssem, rsem, _, _ = gather
        block = ref.at[index, rows_of(z - sign_of(index, way) * distance, role)]
        at = (index, role, way, step)
        return remote(block, block, ssem.at[at], rsem.at[at], target)

    def gather_send(gather, index, role, way, step):
        if (role, way) == FAR and step == 2:
            return gather_copy(gather, index, role, way, step, 2, far(index, way))
        return gather_copy(gather, index, role, way, step, step + role, near(index, way))

    def gather_take(gather, index, role, way, step):
        return gather_copy(gather, index, role, way, step, step + role + 1, near(index, way))

    def gather_cross(gather, index, kind, role):
        ref, _, _, ssem, rsem = gather
        distance = 0 if kind == 2 else sign_of(index, kind)
        block = ref.at[index, rows_of(z - distance, role)]
        return remote(block, block, ssem.at[index, kind], rsem.at[index, kind], pair)

    def gather_first(gather, index):
        for way in range(2):
            gather_send(gather, index, 0, way, 0).start()
        gather_cross(gather, index, 2, 0).start()

    def gather_rest(gather, fill=None):
        for hop in range(1, 5):
            for index in range(3):
                for way in range(2):
                    hops = HOPS[0][way]
                    if hop <= hops:
                        gather_take(gather, index, 0, way, hop - 1).wait_recv()
                        if hop == 1:
                            gather_cross(gather, index, way, 0).start()
                        if hop < hops:
                            gather_send(gather, index, 0, way, hop).start()
                for way in range(2):
                    if hop == 2:
                        gather_cross(gather, index, way, 1).wait_recv()
                        gather_send(gather, index, 1, way, 0).start()
                    if hop == 3:
                        gather_take(gather, index, 1, way, 0).wait_recv()
                        if (1, way) == FAR:
                            gather_send(gather, index, 1, way, 2).start()
                        gather_send(gather, index, 1, way, 1).start()
                    if hop == 4:
                        gather_take(gather, index, 1, way, 1).wait_recv()
                if hop == 2:
                    gather_cross(gather, index, 2, 1).wait_recv()
                if fill is not None:
                    fill()
        for index in range(3):
            gather_take(gather, index, *FAR, 2).wait_recv()

    def gather_drain(gather):
        for index in range(3):
            for way in range(2):
                for role in range(2):
                    for step in range(HOPS[role][way] - role):
                        gather_send(gather, index, role, way, step).wait_send()
            for kind in range(3):
                gather_cross(gather, index, kind, 0).wait_send()

    gather_a = (wa_ref, aga_ssem, aga_rsem, xa_ssem, xa_rsem)
    gather_b = (wb_ref, agb_ssem, agb_rsem, xb_ssem, xb_rsem)
    up_copies = [remote(up_send.at[i], up_recv.at[i], up_ssem.at[i], up_rsem.at[i], across) for i in range(3)]

    @pl.when(jnp.logical_and(upper, seq < last))
    def _():
        for copy in halo:
            copy.start()

    @pl.when(lower)
    def _():
        wa_ref[1] = w0t_ref[1].astype(BF16)
        wa_ref[2] = w0t_ref[2].astype(BF16)
        wdn_ref[...] = w0_ref[0].astype(BF16)
        for index in range(3):
            wc_ref[index] = w0t_ref[index, rows_of(z, 0), :]

    loads[6].wait()

    @pl.when(upper)
    def _():
        attend_own()
        for index in range(3):
            up_copies[index].wait_recv()
            fresh = update(w0t_ref[index, rows_of(z, 0), :], up_recv[index].astype(F32))
            wc_ref[index] = fresh
            wa_ref[index, rows_of(z, 0), :] = fresh.astype(BF16)
            gather_first(gather_a, index)
        gather_rest(gather_a)
        wdn_ref[...] = wa_ref[0].T

    def grad_tile(tile, carry):
        at = pl.multiple_of(tile * TILE, TILE)
        keys = kn_ref[pl.ds(at, TILE), :]
        gate_pre = dot_nt(wa_ref[1], keys)
        up_pre = dot_nt(wa_ref[2], keys)
        rate = rate_ref[0:1, pl.ds(at, TILE)].astype(F32)
        grad = dot_nt(wdn_ref[...], v_ref[pl.ds(at + WINDOW, TILE), :]) * rate
        sig = jax.nn.sigmoid(gate_pre)
        act = gate_pre * sig
        hid_ref[0, :, pl.ds(at, TILE)] = (act * up_pre * rate).astype(BF16)
        hid_ref[1, :, pl.ds(at, TILE)] = (grad * up_pre * sig * (1.0 + gate_pre * (1.0 - sig))).astype(BF16)
        hid_ref[2, :, pl.ds(at, TILE)] = (grad * act).astype(BF16)
        return carry

    lax.fori_loop(0, tiles, grad_tile, 0)

    def sum_copy(index, role, way, step):
        at = (index, role, way, step)
        target = far(index, way) if (role, way) == FAR and step == 0 else near(index, way)
        return remote(rs_send.at[at], rs_recv.at[at], rs_ssem.at[at], rs_rsem.at[at], target)

    def sum_cross(index, kind):
        at = (index, kind)
        return remote(xs_send.at[at], xs_recv.at[at], xs_ssem.at[at], xs_rsem.at[at], pair)

    def sum_step(index, role, way, step):
        hops = HOPS[role][way]
        value = g_ref[index, rows_of(z + sign_of(index, way) * (hops - step), role), :]
        before = [step - 1] if step > 0 else []
        if (role, way) == FAR:
            before = {2: [1, 0], 3: [2]}.get(step, [])
        for earlier in before:
            sum_copy(index, role, way, earlier).wait_recv()
            value = value + rs_recv[index, role, way, earlier].astype(F32)
        if step < hops - 1:
            rs_send[index, role, way, step] = value.astype(BF16)
            sum_copy(index, role, way, step).start()
        elif role == 1:
            xs_send[index, way] = value.astype(BF16)
            sum_cross(index, way).start()
        else:
            sum_cross(index, way).wait_recv()
            value = value + xs_recv[index, way].astype(F32)
            rs_send[index, role, way, step] = value.astype(BF16)
            sum_copy(index, role, way, step).start()

    def scatter_first(index):
        for role in (1, 0):
            for way in (1, 0):
                sum_step(index, role, way, 0)
        sum_step(index, *FAR, 1)
        xs_send[index, 2] = g_ref[index, rows_of(z, 1), :].astype(BF16)
        sum_cross(index, 2).start()

    g_ref[0] = dot_nn(hid_ref[0], v_ref[pl.ds(WINDOW, rows), :]).T
    scatter_first(0)
    g_ref[1] = dot_nn(hid_ref[1], kn_ref[...])
    scatter_first(1)
    g_ref[2] = dot_nn(hid_ref[2], kn_ref[...])
    scatter_first(2)
    for hop in range(1, 4):
        for index in range(3):
            if hop < 3:
                sum_step(index, 1, 0, hop)
            sum_step(index, 0, 0, hop)
            if hop == 1:
                sum_step(index, 0, 1, 1)
            if hop == 3:
                sum_step(index, 0, 1, 2)
        if hop < 3:
            for index in range(3):
                sum_step(index, 1, 1, hop + 1)
    for index in range(3):
        value = g_ref[index, rows_of(z, 0), :]
        sum_cross(index, 2).wait_recv()
        value = value + xs_recv[index, 2].astype(F32)
        for way in range(2):
            final = HOPS[0][way] - 1
            sum_copy(index, 0, way, final).wait_recv()
            value = value + rs_recv[index, 0, way, final].astype(F32)

        @pl.when(lower)
        def _():
            up_send[index] = value.astype(BF16)
            up_copies[index].start()

        wb_ref[index, rows_of(z, 0), :] = update(wc_ref[index], value).astype(BF16)
        gather_first(gather_b, index)

    @pl.when(lower)
    def _():
        for index in range(3):
            up_copies[index].wait_send()
        for copy in halo:
            copy.start()

    @pl.when(upper)
    def _():
        halo_ready()

    slots = [(tile, a) for tile in range(inner) for a in range(heads)]

    def fill():
        if slots:
            tile, a = slots.pop(0)

            @pl.when(upper)
            def _():
                attend(tile, a)

    gather_rest(gather_b, fill)
    while slots:
        fill()

    @pl.when(lower)
    def _():
        attend_own()

        @pl.when(seq > 0)
        def _():
            halo_ready()

        lax.fori_loop(0, inner, attend_tile, 0)

    out_copies = []

    def apply_tile(tile, carry):
        at = pl.multiple_of(tile * TILE, TILE)
        queries = norm_rows(q_ref[pl.ds(at, TILE), :])
        gate_pre = dot_nt(queries, wb_ref[1])
        up_pre = dot_nt(queries, wb_ref[2])
        hidden = (gate_pre * jax.nn.sigmoid(gate_pre) * up_pre).astype(BF16)
        fast = dot_nt(hidden, wb_ref[0]).astype(BF16)
        out_ref[pl.ds(at, TILE), :] = (fast.astype(F32) + att_ref[pl.ds(at, TILE), :]).astype(BF16)
        return carry

    lax.fori_loop(0, tiles, apply_tile, 0)

    gather_drain(gather_b)

    @pl.when(upper)
    def _():
        gather_drain(gather_a)

    for index in range(3):
        for way in range(2):
            for role in range(2):
                for step in range(HOPS[role][way] - role):
                    sum_copy(index, role, way, step).wait_send()
        for kind in range(3):
            sum_cross(index, kind).wait_send()

    @pl.when(seq < last)
    def _():
        for copy in halo:
            copy.wait_send()


def on_device(queries, key_rows, value_rows, learn_rates, gate_fast, down_fast, up_fast):
    rows, width = queries.shape
    chunk = width // NZ
    dma = pltpu.SemaphoreType.DMA
    square = (3, width, width)
    piece = chunk // 2
    sems = (3, 2, 2, 4)
    return pl.pallas_call(
        kernel,
        name="layer",
        out_shape=jax.ShapeDtypeStruct((rows, width), BF16),
        in_specs=[pl.BlockSpec(memory_space=pl.ANY)] * 7,
        out_specs=pl.BlockSpec(memory_space=pltpu.VMEM),
        scratch_shapes=[
            pltpu.VMEM((rows, width), BF16),
            pltpu.VMEM((WINDOW + rows, width), BF16),
            pltpu.VMEM((WINDOW + rows, width), BF16),
            pltpu.VMEM((1, rows), BF16),
            pltpu.VMEM(square, F32),
            pltpu.VMEM(square, F32),
            pltpu.VMEM((rows, width), BF16),
            pltpu.VMEM(square, BF16),
            pltpu.VMEM(square[1:], BF16),
            pltpu.VMEM(square, BF16),
            pltpu.VMEM((3, piece, width), F32),
            pltpu.VMEM((3, width, rows), BF16),
            pltpu.VMEM(square, F32),
            pltpu.VMEM(sems + (piece, width), BF16),
            pltpu.VMEM(sems + (piece, width), BF16),
            pltpu.VMEM((3, 3, piece, width), BF16),
            pltpu.VMEM((3, 3, piece, width), BF16),
            pltpu.VMEM((3, piece, width), BF16),
            pltpu.VMEM((3, piece, width), BF16),
            pltpu.VMEM((rows, width), F32),
            dma((7,)),
            dma((2,)),
            dma((2,)),
            dma(sems),
            dma(sems),
            dma((3, 3)),
            dma((3, 3)),
            dma((3,)),
            dma((3,)),
            dma(sems),
            dma(sems),
            dma((3, 3)),
            dma((3, 3)),
            dma(sems),
            dma(sems),
            dma((3, 3)),
            dma((3, 3)),
        ],
        compiler_params=pltpu.CompilerParams(
            collective_id=0, has_side_effects=True, vmem_limit_bytes=44 * 1024 * 1024
        ),
    )(
        *(
            pltpu.with_memory_space_constraint(array, pltpu.HBM)
            for array in (queries, key_rows, value_rows, learn_rates.T, gate_fast, down_fast, up_fast)
        )
    )


def solution(mesh):
    return jax.shard_map(
        on_device,
        mesh=mesh,
        in_specs=(
            P("seq", "head"),
            P("seq", "head"),
            P("seq", "head"),
            P("seq", "head"),
            P("head", None, None),
            P("head", None, None),
            P("head", None, None),
        ),
        out_specs=P("seq", "head"),
        check_vma=False,
    )
```

```python
import functools
import math

import jax
import jax.numpy as jnp
from jax import lax
from jax.experimental import pallas as pl
from jax.experimental.pallas import tpu as pltpu
from jax.sharding import PartitionSpec as P

AH = 128
WINDOW = 512
TILE = 256
NZ = 8
NY = 4
EPSILON = 1e-06
MESH = pl.DeviceIdType.MESH
HOPS = ((4, 3), (3, 4))
FAR = (1, 1)
F32 = jnp.float32
BF16 = jnp.bfloat16


def dot_nn(a, b):
    return lax.dot_general(a, b, (((1,), (0,)), ((), ())), preferred_element_type=F32)


def dot_nt(a, b):
    return lax.dot_general(a, b, (((1,), (1,)), ((), ())), preferred_element_type=F32)


def norm_rows(rows):
    as_float = rows.astype(F32)
    mean = jnp.mean(as_float * as_float, axis=-1, keepdims=True)
    return (as_float / jnp.sqrt(mean + EPSILON)).astype(BF16)


def kernel(
    q_hbm, k_hbm, v_hbm, rate_hbm, gate_hbm, down_hbm, up_hbm, out_ref,
    q_ref, k_ref, v_ref, rate_ref, w0_ref, w0t_ref, kn_ref, wa_ref, wdn_ref, wb_ref, wc_ref,
    hid_ref, g_ref, rs_send, rs_recv, xs_send, xs_recv, up_send, up_recv, att_ref,
    load_sem, halo_ssem, halo_rsem, rs_ssem, rs_rsem, xs_ssem, xs_rsem, up_ssem, up_rsem,
    aga_ssem, aga_rsem, xa_ssem, xa_rsem, agb_ssem, agb_rsem, xb_ssem, xb_rsem,
):
    rows, width = q_hbm.shape
    chunk = width // NZ
    piece = chunk // 2
    head = lax.axis_index("head")
    seq = lax.axis_index("seq")
    y = seq // NZ
    z = seq % NZ
    upper = y >= NY // 2
    lower = y < NY // 2
    last = NZ * NY - 1
    z_next = y * NZ + lax.rem(z + 1, NZ)
    z_prev = y * NZ + lax.rem(z + NZ - 1, NZ)
    pair = (y + 1 - 2 * lax.rem(y, 2)) * NZ + z
    across = (NY - 1 - y) * NZ + z
    heads = width // AH
    home = jnp.minimum(lax.rem(y, 3), 1)
    part_of = (home, 1 - home)
    tiles = rows // TILE

    def signal(target):
        pl.semaphore_signal(pltpu.get_barrier_semaphore(), inc=1, device_id=(head, target), device_id_type=MESH)

    def remote(src, dst, ssem, rsem, target):
        return pltpu.make_async_remote_copy(
            src_ref=src, dst_ref=dst, send_sem=ssem, recv_sem=rsem, device_id=(head, target), device_id_type=MESH
        )

    loads = [
        pltpu.make_async_copy(k_hbm, k_ref.at[pl.ds(WINDOW, rows)], load_sem.at[0]),
        pltpu.make_async_copy(gate_hbm.at[0], w0_ref.at[1], load_sem.at[1]),
        pltpu.make_async_copy(up_hbm.at[0], w0_ref.at[2], load_sem.at[2]),
        pltpu.make_async_copy(down_hbm.at[0], w0_ref.at[0], load_sem.at[3]),
        pltpu.make_async_copy(v_hbm, v_ref.at[pl.ds(WINDOW, rows)], load_sem.at[4]),
        pltpu.make_async_copy(rate_hbm, rate_ref, load_sem.at[5]),
        pltpu.make_async_copy(q_hbm, q_ref, load_sem.at[6]),
    ]
    for load in (loads[0], loads[1], loads[2], loads[4], loads[5], loads[3]):
        load.start()

    far_next = y * NZ + lax.rem(z + 2, NZ)
    far_prev = y * NZ + lax.rem(z + NZ - 2, NZ)
    for target in (z_next, z_prev, far_next, far_prev, pair, across):
        signal(target)
    edge_next = jnp.logical_and(z == NZ - 1, y < NY - 1)
    edge_prev = jnp.logical_and(z == 0, y > 0)

    @pl.when(edge_next)
    def _():
        signal(seq + 1)

    @pl.when(edge_prev)
    def _():
        signal(seq - 1)

    def norm_keys(tile, carry):
        at = pl.multiple_of(tile * TILE, TILE)
        kn_ref[pl.ds(at, TILE), :] = norm_rows(k_ref[pl.ds(at + WINDOW, TILE), :])
        return carry

    loads[0].wait()
    lax.fori_loop(0, tiles, norm_keys, 0)
    for index, load in ((1, loads[1]), (2, loads[2])):
        load.wait()
        w0t_ref[index] = w0_ref[index].T
    loads[3].wait()
    loads[6].start()
    loads[4].wait()
    loads[5].wait()

    pl.semaphore_wait(
        pltpu.get_barrier_semaphore(), 6 + edge_next.astype(jnp.int32) + edge_prev.astype(jnp.int32)
    )

    halo = [
        remote(
            ref.at[pl.ds(rows, WINDOW)], ref.at[pl.ds(0, WINDOW)], halo_ssem.at[i], halo_rsem.at[i],
            lax.rem(seq + 1, NZ * NY),
        )
        for i, ref in enumerate((k_ref, v_ref))
    ]

    @pl.when(seq == 0)
    def _():
        k_ref[pl.ds(0, WINDOW), :] = jnp.zeros((WINDOW, width), BF16)
        v_ref[pl.ds(0, WINDOW), :] = jnp.zeros((WINDOW, width), BF16)

    def attend(tile, a):
        at = pl.multiple_of(tile * TILE, TILE)
        row = lax.broadcasted_iota(jnp.int32, (TILE, TILE), 0)
        col = lax.broadcasted_iota(jnp.int32, (TILE, TILE), 1)
        recent = col <= row
        real0 = jnp.logical_or(seq > 0, at >= WINDOW)
        real1 = jnp.logical_or(seq > 0, at + TILE >= WINDOW)
        scale = math.log2(math.e) / math.sqrt(AH)
        lanes = slice(a * AH, (a + 1) * AH)
        q = q_ref[pl.ds(at, TILE), lanes]
        s0 = dot_nt(q, k_ref[pl.ds(at, TILE), lanes])
        s1 = dot_nt(q, k_ref[pl.ds(at + TILE, TILE), lanes])
        s2 = dot_nt(q, k_ref[pl.ds(at + 2 * TILE, TILE), lanes])
        edge = jnp.where(recent, s2, jnp.where(real0, s0, -1e30))
        middle = jnp.where(real1, s1, -1e30)
        top = jnp.max(jnp.maximum(edge, middle), axis=-1, keepdims=True)
        edge = jnp.exp2((edge - top) * scale)
        middle = jnp.exp2((middle - top) * scale)
        total = jnp.sum(edge + middle, axis=-1, keepdims=True)
        out = dot_nn(middle.astype(BF16), v_ref[pl.ds(at + TILE, TILE), lanes])
        out += dot_nn(jnp.where(recent, edge, 0.0).astype(BF16), v_ref[pl.ds(at + 2 * TILE, TILE), lanes])
        out += dot_nn(jnp.where(recent, 0.0, edge).astype(BF16), v_ref[pl.ds(at, TILE), lanes])
        att_ref[pl.ds(at, TILE), lanes] = out / total

    def attend_tile(tile, carry):
        for a in range(heads):
            attend(tile, a)
        return carry

    inner = WINDOW // TILE

    def attend_own():
        lax.fori_loop(inner, tiles, attend_tile, 0)

    def halo_ready():
        for copy in halo:
            copy.wait_recv()

    def update(old, step):
        moved = old + step
        before = jnp.sum(old * old, axis=-1, keepdims=True)
        after = jnp.sum(moved * moved, axis=-1, keepdims=True)
        return moved * (jnp.sqrt(before) / jnp.sqrt(after + EPSILON))

    def rows_of(position, role):
        start = lax.rem(position + 2 * NZ, NZ) * chunk + part_of[role] * piece
        return pl.ds(pl.multiple_of(start, piece), piece)

    def sign_of(index, way):
        return 1 if (way + index) % 2 == 0 else -1

    def near(index, way):
        return z_next if sign_of(index, way) > 0 else z_prev

    def far(index, way):
        return far_next if sign_of(index, way) > 0 else far_prev

    def gather_copy(gather, index, role, way, step, distance, target):
        ref, ssem, rsem, _, _ = gather
        block = ref.at[index, rows_of(z - sign_of(index, way) * distance, role)]
        at = (index, role, way, step)
        return remote(block, block, ssem.at[at], rsem.at[at], target)

    def gather_send(gather, index, role, way, step):
        if (role, way) == FAR and step == 2:
            return gather_copy(gather, index, role, way, step, 2, far(index, way))
        return gather_copy(gather, index, role, way, step, step + role, near(index, way))

    def gather_take(gather, index, role, way, step):
        return gather_copy(gather, index, role, way, step, step + role + 1, near(index, way))

    def gather_cross(gather, index, kind, role):
        ref, _, _, ssem, rsem = gather
        distance = 0 if kind == 2 else sign_of(index, kind)
        block = ref.at[index, rows_of(z - distance, role)]
        return remote(block, block, ssem.at[index, kind], rsem.at[index, kind], pair)

    def gather_first(gather, index):
        for way in range(2):
            gather_send(gather, index, 0, way, 0).start()
        gather_cross(gather, index, 2, 0).start()

    def gather_rest(gather, fill=None):
        for hop in range(1, 5):
            for index in range(3):
                for way in range(2):
                    hops = HOPS[0][way]
                    if hop <= hops:
                        gather_take(gather, index, 0, way, hop - 1).wait_recv()
                        if hop == 1:
                            gather_cross(gather, index, way, 0).start()
                        if hop < hops:
                            gather_send(gather, index, 0, way, hop).start()
                for way in range(2):
                    if hop == 2:
                        gather_cross(gather, index, way, 1).wait_recv()
                        gather_send(gather, index, 1, way, 0).start()
                    if hop == 3:
                        gather_take(gather, index, 1, way, 0).wait_recv()
                        if (1, way) == FAR:
                            gather_send(gather, index, 1, way, 2).start()
                        gather_send(gather, index, 1, way, 1).start()
                    if hop == 4:
                        gather_take(gather, index, 1, way, 1).wait_recv()
                if hop == 2:
                    gather_cross(gather, index, 2, 1).wait_recv()
                if fill is not None:
                    fill()
        for index in range(3):
            gather_take(gather, index, *FAR, 2).wait_recv()

    def gather_drain(gather):
        for index in range(3):
            for way in range(2):
                for role in range(2):
                    for step in range(HOPS[role][way] - role):
                        gather_send(gather, index, role, way, step).wait_send()
            for kind in range(3):
                gather_cross(gather, index, kind, 0).wait_send()

    gather_a = (wa_ref, aga_ssem, aga_rsem, xa_ssem, xa_rsem)
    gather_b = (wb_ref, agb_ssem, agb_rsem, xb_ssem, xb_rsem)
    up_copies = [remote(up_send.at[i], up_recv.at[i], up_ssem.at[i], up_rsem.at[i], across) for i in range(3)]

    @pl.when(jnp.logical_and(upper, seq < last))
    def _():
        for copy in halo:
            copy.start()

    @pl.when(lower)
    def _():
        wa_ref[1] = w0t_ref[1].astype(BF16)
        wa_ref[2] = w0t_ref[2].astype(BF16)
        wdn_ref[...] = w0_ref[0].astype(BF16)

    @pl.when(upper)
    def _():
        w0t_ref[0] = w0_ref[0].T
        loads[6].wait()
        attend_own()
        for index in range(3):
            up_copies[index].wait_recv()
            fresh = update(w0t_ref[index, rows_of(z, 0), :], up_recv[index].astype(F32))
            wc_ref[index] = fresh
            wa_ref[index, rows_of(z, 0), :] = fresh.astype(BF16)
            gather_first(gather_a, index)
        gather_rest(gather_a)
        wdn_ref[...] = wa_ref[0].T

    def grad_tile(tile, carry):
        at = pl.multiple_of(tile * TILE, TILE)
        keys = kn_ref[pl.ds(at, TILE), :]
        gate_pre = dot_nt(wa_ref[1], keys)
        up_pre = dot_nt(wa_ref[2], keys)
        rate = rate_ref[0:1, pl.ds(at, TILE)].astype(F32)
        grad = dot_nt(wdn_ref[...], v_ref[pl.ds(at + WINDOW, TILE), :]) * rate
        sig = jax.nn.sigmoid(gate_pre)
        act = gate_pre * sig
        hid_ref[0, :, pl.ds(at, TILE)] = (act * up_pre * rate).astype(BF16)
        hid_ref[1, :, pl.ds(at, TILE)] = (grad * up_pre * sig * (1.0 + gate_pre * (1.0 - sig))).astype(BF16)
        hid_ref[2, :, pl.ds(at, TILE)] = (grad * act).astype(BF16)
        return carry

    lax.fori_loop(0, tiles, grad_tile, 0)

    def sum_copy(index, role, way, step):
        at = (index, role, way, step)
        target = far(index, way) if (role, way) == FAR and step == 0 else near(index, way)
        return remote(rs_send.at[at], rs_recv.at[at], rs_ssem.at[at], rs_rsem.at[at], target)

    def sum_cross(index, kind):
        at = (index, kind)
        return remote(xs_send.at[at], xs_recv.at[at], xs_ssem.at[at], xs_rsem.at[at], pair)

    def sum_step(index, role, way, step):
        hops = HOPS[role][way]
        value = g_ref[index, rows_of(z + sign_of(index, way) * (hops - step), role), :]
        before = [step - 1] if step > 0 else []
        if (role, way) == FAR:
            before = {2: [1, 0], 3: [2]}.get(step, [])
        for earlier in before:
            sum_copy(index, role, way, earlier).wait_recv()
            value = value + rs_recv[index, role, way, earlier].astype(F32)
        if step < hops - 1:
            rs_send[index, role, way, step] = value.astype(BF16)
            sum_copy(index, role, way, step).start()
        elif role == 1:
            xs_send[index, way] = value.astype(BF16)
            sum_cross(index, way).start()
        else:
            sum_cross(index, way).wait_recv()
            value = value + xs_recv[index, way].astype(F32)
            rs_send[index, role, way, step] = value.astype(BF16)
            sum_copy(index, role, way, step).start()

    def scatter_first(index):
        for role in (1, 0):
            for way in (1, 0):
                sum_step(index, role, way, 0)
        sum_step(index, *FAR, 1)
        xs_send[index, 2] = g_ref[index, rows_of(z, 1), :].astype(BF16)
        sum_cross(index, 2).start()

    g_ref[0] = dot_nn(hid_ref[0], v_ref[pl.ds(WINDOW, rows), :]).T
    scatter_first(0)
    g_ref[1] = dot_nn(hid_ref[1], kn_ref[...])
    scatter_first(1)
    g_ref[2] = dot_nn(hid_ref[2], kn_ref[...])
    scatter_first(2)

    @pl.when(lower)
    def _():
        w0t_ref[0] = w0_ref[0].T
        for index in range(3):
            wc_ref[index] = w0t_ref[index, rows_of(z, 0), :]

    for hop in range(1, 4):
        for index in range(3):
            if hop < 3:
                sum_step(index, 1, 0, hop)
            sum_step(index, 0, 0, hop)
            if hop == 1:
                sum_step(index, 0, 1, 1)
            if hop == 3:
                sum_step(index, 0, 1, 2)
        if hop < 3:
            for index in range(3):
                sum_step(index, 1, 1, hop + 1)
    for index in range(3):
        value = g_ref[index, rows_of(z, 0), :]
        sum_cross(index, 2).wait_recv()
        value = value + xs_recv[index, 2].astype(F32)
        for way in range(2):
            final = HOPS[0][way] - 1
            sum_copy(index, 0, way, final).wait_recv()
            value = value + rs_recv[index, 0, way, final].astype(F32)

        @pl.when(lower)
        def _():
            up_send[index] = value.astype(BF16)
            up_copies[index].start()

        wb_ref[index, rows_of(z, 0), :] = update(wc_ref[index], value).astype(BF16)
        gather_first(gather_b, index)

    @pl.when(lower)
    def _():
        for index in range(3):
            up_copies[index].wait_send()
        for copy in halo:
            copy.start()

    @pl.when(upper)
    def _():
        halo_ready()

    slots = [(tile, a) for tile in range(inner) for a in range(heads)]

    def fill():
        if slots:
            tile, a = slots.pop(0)

            @pl.when(upper)
            def _():
                attend(tile, a)

    gather_rest(gather_b, fill)
    while slots:
        fill()

    @pl.when(lower)
    def _():
        loads[6].wait()
        attend_own()

        @pl.when(seq > 0)
        def _():
            halo_ready()

        lax.fori_loop(0, inner, attend_tile, 0)

    out_copies = []

    def apply_tile(tile, carry):
        at = pl.multiple_of(tile * TILE, TILE)
        queries = norm_rows(q_ref[pl.ds(at, TILE), :])
        gate_pre = dot_nt(queries, wb_ref[1])
        up_pre = dot_nt(queries, wb_ref[2])
        hidden = (gate_pre * jax.nn.sigmoid(gate_pre) * up_pre).astype(BF16)
        fast = dot_nt(hidden, wb_ref[0]).astype(BF16)
        out_ref[pl.ds(at, TILE), :] = (fast.astype(F32) + att_ref[pl.ds(at, TILE), :]).astype(BF16)
        return carry

    lax.fori_loop(0, tiles, apply_tile, 0)

    gather_drain(gather_b)

    @pl.when(upper)
    def _():
        gather_drain(gather_a)

    for index in range(3):
        for way in range(2):
            for role in range(2):
                for step in range(HOPS[role][way] - role):
                    sum_copy(index, role, way, step).wait_send()
        for kind in range(3):
            sum_cross(index, kind).wait_send()

    @pl.when(seq < last)
    def _():
        for copy in halo:
            copy.wait_send()


def on_device(queries, key_rows, value_rows, learn_rates, gate_fast, down_fast, up_fast):
    rows, width = queries.shape
    chunk = width // NZ
    dma = pltpu.SemaphoreType.DMA
    square = (3, width, width)
    piece = chunk // 2
    sems = (3, 2, 2, 4)
    return pl.pallas_call(
        kernel,
        name="layer",
        out_shape=jax.ShapeDtypeStruct((rows, width), BF16),
        in_specs=[pl.BlockSpec(memory_space=pl.ANY)] * 7,
        out_specs=pl.BlockSpec(memory_space=pltpu.VMEM),
        scratch_shapes=[
            pltpu.VMEM((rows, width), BF16),
            pltpu.VMEM((WINDOW + rows, width), BF16),
            pltpu.VMEM((WINDOW + rows, width), BF16),
            pltpu.VMEM((1, rows), BF16),
            pltpu.VMEM(square, F32),
            pltpu.VMEM(square, F32),
            pltpu.VMEM((rows, width), BF16),
            pltpu.VMEM(square, BF16),
            pltpu.VMEM(square[1:], BF16),
            pltpu.VMEM(square, BF16),
            pltpu.VMEM((3, piece, width), F32),
            pltpu.VMEM((3, width, rows), BF16),
            pltpu.VMEM(square, F32),
            pltpu.VMEM(sems + (piece, width), BF16),
            pltpu.VMEM(sems + (piece, width), BF16),
            pltpu.VMEM((3, 3, piece, width), BF16),
            pltpu.VMEM((3, 3, piece, width), BF16),
            pltpu.VMEM((3, piece, width), BF16),
            pltpu.VMEM((3, piece, width), BF16),
            pltpu.VMEM((rows, width), F32),
            dma((7,)),
            dma((2,)),
            dma((2,)),
            dma(sems),
            dma(sems),
            dma((3, 3)),
            dma((3, 3)),
            dma((3,)),
            dma((3,)),
            dma(sems),
            dma(sems),
            dma((3, 3)),
            dma((3, 3)),
            dma(sems),
            dma(sems),
            dma((3, 3)),
            dma((3, 3)),
        ],
        compiler_params=pltpu.CompilerParams(
            collective_id=0, has_side_effects=True, vmem_limit_bytes=44 * 1024 * 1024
        ),
    )(
        *(
            pltpu.with_memory_space_constraint(array, pltpu.HBM)
            for array in (queries, key_rows, value_rows, learn_rates.T, gate_fast, down_fast, up_fast)
        )
    )


def solution(mesh):
    return jax.shard_map(
        on_device,
        mesh=mesh,
        in_specs=(
            P("seq", "head"),
            P("seq", "head"),
            P("seq", "head"),
            P("seq", "head"),
            P("head", None, None),
            P("head", None, None),
            P("head", None, None),
        ),
        out_specs=P("seq", "head"),
        check_vma=False,
    )
```
